32 devices in a mesh: seq: 8 (over y, x, core), exp: 4 (over z).
Axes of the slice: x: 2, y: 2, z: 4, core: 2. Of those that a mesh axis runs over, the one named last changes fastest.
Arguments:
- queries: bfloat16 [2048, 4096], P('seq', 'exp'), may hold values from -6 to 6
- key_rows: bfloat16 [2048, 512], P('seq'), may hold values from -6 to 6
- value_rows: bfloat16 [2048, 512], P('seq'), may hold values from -6 to 6
- sink_logits: float32 [64], P('exp'), may hold values from -2 to 2
- residual: bfloat16 [2048, 2880], P('seq'), may hold values from -6 to 6
- out_weight: bfloat16 [4096, 2880], P('exp'), may hold values from -0.375 to 0.375
- norm_gain: float32 [2880], replicated, may hold values from 0.25 to 1.75
- expert_ids: int32 [2048, 4], P('seq'), may hold values from 0 to 31, all different within a row; in each aligned block of 256 rows (0 to 255, 256 to 511, ...) at most 48 rows name the same one
- route_gates: float32 [2048, 4], P('seq'), may hold values from 0.1 to 0.6
- gate_proj: bfloat16 [32, 2880, 2048], P('seq', None, 'exp'), may hold values from -0.109375 to 0.109375
- up_proj: bfloat16 [32, 2880, 2048], P('seq', None, 'exp'), may hold values from -0.109375 to 0.109375
- down_proj: bfloat16 [32, 2048, 2880], P('seq', 'exp'), may hold values from -0.125 to 0.125
Outputs:
- layer_out: bfloat16 [2048, 2880], P('seq')
The draws below stay inside these ranges and needn't reach their ends.
Inputs may be any that keep to these rules, and one draw needn't show every extreme that they name: `expert_ids`: each token names 4 different experts. In each slab of 256 tokens no expert is named by more than 48 entries, and that bound is reached.
All inputs are finite; a program needn't handle non-finite values.
Results may differ from the reference program's by a relative error of at most 0.018.
Values may be sent and summed in bfloat16 or wider, within the bound.
No kernel may reach another device: no remote copies, remote signals or barrier semaphores. Data moves between devices by JAX's collectives and lax.ppermute only.
A program may use at most 128 MiB of HBM per device.

```python
import math
import jax
import jax.numpy as jnp
import numpy as np
from jax import lax

D = 2880
HQ = 64
HK = 8
HEAD = 64
TOP = 4
WIN = 128
FF = 2048
SLAB = 256
SEQ_LEN = 2048
EXPERTS = 32
CAP = 48
N_EXP = 4


def draw_queries(key, part):
    base_key = jax.random.fold_in(key, 1)
    fresh = jnp.clip(jax.random.normal(base_key, (SEQ_LEN, HQ * HEAD), jnp.float32), -4.0, 4.0)
    return fresh.astype(jnp.bfloat16)


def draw_key_rows(key, part):
    base_key = jax.random.fold_in(key, 2)
    fresh = jnp.clip(jax.random.normal(base_key, (SEQ_LEN, HK * HEAD), jnp.float32), -4.0, 4.0)
    return fresh.astype(jnp.bfloat16)


def steps_of(key, dims, shards, low, top_value):
    loudness, own = 1.0, jax.random.fold_in(key, 6)
    for axis_at, shards_of in shards:
        draws = jnp.exp(jax.random.uniform(jax.random.fold_in(own, axis_at), (shards_of,), jnp.float32, low / len(shards), top_value / len(shards)))
        loudness = loudness * jnp.repeat(draws, dims[axis_at] // shards_of).reshape([-1 if axis == axis_at else 1 for axis in range(len(dims))])
    return loudness


def shared_out(own_key, own, number, rows, amount, top, bound, lean):
    sequence = jax.random.permutation(own_key, amount)
    packed, usual = shares(amount, rows * top, bound, lean, True), shares(amount, rows * top, bound, lean, False)
    places = jnp.arange(amount)

    def named(lengths, rotation):
        used = int((lengths > 0).sum())
        fixed = max(1, used // 4)
        passed = fixed + (places - fixed + rotation * (used - fixed)) % max(1, amount - fixed)
        return jnp.zeros((amount,), jnp.int32).at[sequence[jnp.where(places < fixed, places, passed)]].set(jnp.asarray(lengths, jnp.int32))

    lengths = jnp.where(number % 4 == 0, named(packed, number // 4), named(usual, number - number // 4 - 1))
    mixed = jax.random.permutation(jax.random.fold_in(own, 3), amount)
    source_of, sink = mixed[0:amount // 2 * 2:2], mixed[1:amount // 2 * 2:2]
    margin = jnp.minimum(lengths[source_of] - 1, bound - lengths[sink]) // 2
    margin = jnp.where((source_of == sequence[0]) | (sink == sequence[0]) | (lengths[sink] == 0), 0, jnp.maximum(margin, 0))
    passed = jax.random.randint(jax.random.fold_in(own, 4), (amount // 2,), 0, 1 << 20) % (margin + 1)
    lengths = lengths.at[source_of].add(-passed).at[sink].add(passed)
    members = jnp.searchsorted(jnp.cumsum(lengths), jnp.arange(rows * top), side="right").astype(jnp.int32)
    table = members.reshape(top, rows).T
    table = table[jax.random.permutation(jax.random.fold_in(own, 1), rows)]
    rotation = jax.random.randint(jax.random.fold_in(own, 2), (rows, 1), 0, top)
    return jnp.take_along_axis(table, (jnp.arange(top)[None, :] + rotation) % top, axis=1)


def shares(number_of, total, bound, lean, full):
    portions = [(1 << 20) // math.isqrt(grade ** lean) + 1 for grade in range(1, number_of + 1)]
    largest = bound if full else min(bound, max(-(-total // number_of), total * portions[0] // sum(portions)))
    least = 1 if total - largest >= number_of - 1 else 0
    holding, surplus = [largest] + [least] * (number_of - 1), total - largest - least * (number_of - 1)
    while surplus > 0:
        candidates = [i for i in range(1, number_of) if holding[i] < largest] or [i for i in range(1, number_of) if holding[i] < bound]
        whole, left = sum([portions[i] for i in candidates]), surplus
        for i in candidates:
            more = min(bound - holding[i], max(1, left * portions[i] // whole), surplus)
            holding[i] = holding[i] + more
            surplus = surplus - more
    return np.array(holding)


def normal_values(rng, shape, width, reach, cuts=(), kind=jnp.bfloat16):
    entries = width * jax.random.normal(rng, shape, jnp.float32)
    if cuts:
        entries = entries * steps_of(rng, shape, cuts, -0.22, 0.18)
    return jnp.clip(entries, -reach, reach).astype(kind)


def setup_inputs(seed: int = 0) -> dict:
    splits = jax.random.split(jax.random.key(seed), 13)
    queries = draw_queries(jax.random.fold_in(splits[12], 71), 0)
    key_rows = draw_key_rows(jax.random.fold_in(splits[12], 71), 0)
    value_rows = normal_values(splits[2], (SEQ_LEN, HK * HEAD), 1.0, 6.0, ((0, 8),))
    sink_logits = jnp.clip(jax.random.uniform(splits[3], (HQ,), jnp.float32, -2.0, 2.0) * steps_of(splits[3], (HQ,), ((0, 4),), -0.4, 0.0), -2.0, 2.0)
    residual = normal_values(splits[4], (SEQ_LEN, D), 1.0, 6.0, ((0, 8),))
    out_weight = normal_values(splits[5], (HQ * HEAD, D), (HQ * HEAD // 16) ** -0.5, 0.375, ((0, 4),))
    norm_gain = jnp.clip(1.0 + 0.15 * jax.random.normal(splits[6], (D,), jnp.float32), 0.25, 1.75)
    expert_ids_keys = jax.random.split(jax.random.fold_in(splits[7], 1), SEQ_LEN // SLAB)
    expert_ids_turns = jax.random.permutation(jax.random.fold_in(splits[7], 3), SEQ_LEN // SLAB)
    expert_ids = jax.vmap(lambda own, number: shared_out(jax.random.fold_in(splits[7], 2), own, number, SLAB, EXPERTS, TOP, CAP, 2))(expert_ids_keys, expert_ids_turns).reshape((SEQ_LEN, TOP))
    route_gates = jnp.clip(0.1 + 0.5 * jax.random.uniform(splits[8], (SEQ_LEN, TOP), jnp.float32) ** steps_of(splits[8], (SEQ_LEN, TOP), ((0, 8),), -0.2, 0.2), 0.1, 0.6)
    gate_proj = normal_values(splits[9], (EXPERTS, D, FF), D ** -0.5, 0.109375, ((0, 8), (2, 4)))
    up_proj = normal_values(splits[10], (EXPERTS, D, FF), D ** -0.5, 0.109375, ((0, 8), (2, 4)))
    down_proj = normal_values(splits[11], (EXPERTS, FF, D), FF ** -0.5, 0.125, ((0, 8), (1, 4)))
    return dict(queries=queries, key_rows=key_rows, value_rows=value_rows, sink_logits=sink_logits, residual=residual, out_weight=out_weight, norm_gain=norm_gain, expert_ids=expert_ids, route_gates=route_gates, gate_proj=gate_proj, up_proj=up_proj, down_proj=down_proj)


def normalize(mixed, gain):
    wide_vals = mixed.astype(jnp.float32)
    inv_scale = lax.rsqrt(lax.optimization_barrier(jnp.mean(wide_vals * wide_vals, axis=-1, keepdims=True)) + 1e-05)
    return (wide_vals * inv_scale * gain).astype(jnp.bfloat16)

def activate(gate_acc, up_acc):
    gate_acc = jnp.minimum(gate_acc, 7.0)
    up_acc = jnp.clip(up_acc, -7.0, 7.0)
    return ((up_acc + 1.0) * gate_acc * jax.nn.sigmoid(1.702 * gate_acc)).astype(jnp.bfloat16)

def slot_numbers(flat_ids, experts):
    onehot = (flat_ids[:, None] == jnp.arange(experts, dtype=jnp.int32)[None, :]).astype(jnp.int32)
    rank_ids = jnp.cumsum(onehot, axis=0) - 1
    return lax.optimization_barrier(jnp.sum(rank_ids * onehot, axis=1)).astype(jnp.int32)

def reference(queries, key_rows, value_rows, sink_logits, residual, out_weight, norm_gain, expert_ids, route_gates, gate_proj, up_proj, down_proj):
    per_group = HQ // HK
    slab_count = SEQ_LEN // SLAB
    q_slabs = queries.reshape(slab_count, SLAB, HQ, HEAD)
    k_slabs = key_rows.reshape(slab_count, SLAB, HK, HEAD)
    v_slabs = value_rows.reshape(slab_count, SLAB, HK, HEAD)
    zero_tail = jnp.zeros((1, WIN, HK, HEAD), jnp.bfloat16)
    k_full = jnp.concatenate([jnp.concatenate([zero_tail, k_slabs[:-1, SLAB - WIN:]], 0), k_slabs], 1)
    v_full = jnp.concatenate([jnp.concatenate([zero_tail, v_slabs[:-1, SLAB - WIN:]], 0), v_slabs], 1)
    factor = 1.0 / math.sqrt(HEAD)

    def one_slab(inputs):
        q_block, k_block, v_block, first_pos = inputs
        k_heads = jnp.repeat(k_block, per_group, axis=1).astype(jnp.float32)
        v_heads = jnp.repeat(v_block, per_group, axis=1).astype(jnp.float32)
        scores = jnp.einsum('qhd,khd->hqk', q_block.astype(jnp.float32), k_heads) * factor
        q_pos = first_pos + jnp.arange(SLAB, dtype=jnp.int32)
        k_pos = first_pos - WIN + jnp.arange(WIN + SLAB, dtype=jnp.int32)
        allowed = (k_pos[None, :] <= q_pos[:, None]) & (k_pos[None, :] > q_pos[:, None] - WIN) & (k_pos[None, :] >= 0)
        scores = jnp.where(allowed[None], scores, -1e+30)
        row_top = jnp.maximum(lax.optimization_barrier(jnp.max(scores, axis=-1)), sink_logits[:, None])
        expo = jnp.exp(scores - row_top[..., None])
        denominator = lax.optimization_barrier(jnp.sum(expo, axis=-1)) + jnp.exp(sink_logits[:, None] - row_top)
        weights = (expo / denominator[..., None]).astype(jnp.bfloat16)
        context = jnp.einsum('hqk,khd->qhd', weights.astype(jnp.float32), v_heads)
        return context.astype(jnp.bfloat16).reshape(SLAB, HQ * HEAD)
    starts = jnp.arange(slab_count, dtype=jnp.int32) * SLAB
    context = lax.map(one_slab, (q_slabs, k_full, v_full, starts)).reshape(SEQ_LEN, HQ * HEAD)
    attn_out = jnp.dot(context, out_weight, preferred_element_type=jnp.float32)
    mixed = (residual.astype(jnp.float32) + attn_out).astype(jnp.bfloat16)
    normed = normalize(mixed, norm_gain)
    flat_ids = expert_ids.reshape(slab_count, SLAB * TOP).astype(jnp.int32)
    slot_ids = jax.vmap(lambda row_ids: slot_numbers(row_ids, EXPERTS))(flat_ids)
    token_of = jnp.arange(SLAB * TOP, dtype=jnp.int32) // TOP
    source_ids = jnp.arange(slab_count, dtype=jnp.int32)[:, None]
    target_rows = ((flat_ids * slab_count + source_ids) * CAP + slot_ids).reshape(-1)
    normed_slabs = normed.reshape(slab_count, SLAB, D)
    entry_rows = normed_slabs[:, token_of].reshape(-1, D)
    buffer = jnp.zeros((EXPERTS * slab_count * CAP, D), jnp.bfloat16).at[target_rows].set(entry_rows)
    buffer = buffer.reshape(EXPERTS, slab_count * CAP, D)
    blocks = FF // N_EXP

    def one_expert(inputs):
        slot_rows, w_gate, w_up, w_down = inputs
        gate_acc = jnp.dot(slot_rows, w_gate, preferred_element_type=jnp.float32)
        up_acc = jnp.dot(slot_rows, w_up, preferred_element_type=jnp.float32)
        hidden = activate(gate_acc, up_acc)
        hidden_blocks = hidden.reshape(-1, N_EXP, blocks).astype(jnp.float32)
        down_blocks = w_down.reshape(N_EXP, blocks, D).astype(jnp.float32)
        parts = jnp.einsum('rbf,bfd->brd', hidden_blocks, down_blocks).astype(jnp.bfloat16)
        parts = lax.optimization_barrier(parts)
        return lax.optimization_barrier(jnp.sum(parts.astype(jnp.float32), axis=0))
    expert_out = lax.map(one_expert, (buffer, gate_proj, up_proj, down_proj)).reshape(-1, D)
    picked = expert_out[target_rows].reshape(SEQ_LEN, TOP, D)
    moe = lax.optimization_barrier(jnp.sum(picked * route_gates[:, :, None], axis=1))
    return (mixed.astype(jnp.float32) + moe).astype(jnp.bfloat16)
```

```python
import functools
import math

import jax
import jax.numpy as jnp
from jax import lax
from jax.experimental import pallas as pl
from jax.experimental.pallas import tpu as pltpu
from jax.sharding import PartitionSpec as P

HQ = 64
HK = 8
HEAD = 64
TOP = 4
WIN = 128
LANES = 128
F32 = jnp.float32
BF16 = jnp.bfloat16
VMEM_BYTES = 56 * 1024 * 1024


def params(*semantics):
    return pltpu.CompilerParams(dimension_semantics=semantics, vmem_limit_bytes=VMEM_BYTES)


def cost(flops, nbytes):
    return pl.CostEstimate(flops=int(flops), bytes_accessed=int(nbytes), transcendentals=0)


def full(shape):
    zeros = (0,) * len(shape)
    return pl.BlockSpec(shape, lambda *_: zeros)


def swap(x, axis, bit):
    count = lax.axis_size(axis)
    return lax.ppermute(x, axis, [(i, i ^ bit) for i in range(count)])


def route_kernel(first_ref, meta_ref, place_ref, turned_ref, gate_ref, *, slabs, experts, cap, rows):
    first = first_ref[0].astype(F32)
    masks, gates = [], []
    for n in range(slabs):
        ids = meta_ref[n, 0:TOP, :]
        amounts = meta_ref[n, TOP : 2 * TOP, :]
        for e in range(experts):
            hit = ids == first + e
            masks.append(jnp.max(jnp.where(hit, 1.0, 0.0), axis=0, keepdims=True))
            gates.append(jnp.sum(jnp.where(hit, amounts, 0.0), axis=0, keepdims=True))
    mask = jnp.concatenate(masks, axis=0)
    before = lax.broadcasted_iota(jnp.int32, (rows, rows), 0) < lax.broadcasted_iota(
        jnp.int32, (rows, rows), 1
    )
    earlier = jnp.dot(
        mask.astype(BF16), jnp.where(before, 1.0, 0.0).astype(BF16), preferred_element_type=F32
    )
    slot = jnp.where(mask > 0.0, earlier, -1.0)
    wanted = lax.broadcasted_iota(jnp.int32, (cap, rows), 0).astype(F32)
    for n in range(slabs):
        pieces = []
        for e in range(experts):
            at = n * experts + e
            chosen = jnp.where(slot[at : at + 1, :] == wanted, 1.0, 0.0)
            pieces.append(chosen)
            row_gate = jnp.sum(chosen * gates[at], axis=1, keepdims=True)
            gate_ref[e, n * cap : (n + 1) * cap, :] = jnp.broadcast_to(row_gate, (cap, LANES))
        place = jnp.concatenate(pieces, axis=0)
        place_ref[n] = place.astype(BF16)
        turned_ref[n] = place.T.astype(BF16)


def route(first, meta, experts, cap):
    slabs, _, rows = meta.shape
    return pl.pallas_call(
        functools.partial(route_kernel, slabs=slabs, experts=experts, cap=cap, rows=rows),
        out_shape=(
            jax.ShapeDtypeStruct((slabs, experts * cap, rows), BF16),
            jax.ShapeDtypeStruct((slabs, rows, experts * cap), BF16),
            jax.ShapeDtypeStruct((experts, slabs * cap, LANES), F32),
        ),
        in_specs=[
            pl.BlockSpec(memory_space=pltpu.SMEM),
            pl.BlockSpec(memory_space=pltpu.VMEM),
        ],
        out_specs=[pl.BlockSpec(memory_space=pltpu.VMEM)] * 3,
        compiler_params=pltpu.CompilerParams(vmem_limit_bytes=VMEM_BYTES),
        cost_estimate=cost(4e9, 2e6),
        name="route",
    )(first, meta)


def attention_kernel(slab_ref, sink_ref, q_ref, k_ref, v_ref, out_ref, *, heads, kv_count):
    block = pl.program_id(0)
    span = 2 * WIN
    row = lax.broadcasted_iota(jnp.int32, (WIN, span), 0)
    key = lax.broadcasted_iota(jnp.int32, (WIN, span), 1)
    first_key = jnp.where((slab_ref[0] == 0) & (block == 0), WIN, 0)
    allowed = (key <= row + WIN) & (key > row) & (key >= first_key)
    begin = pl.multiple_of(block * WIN, WIN)
    per_kv = heads // kv_count
    for pair in range(heads // 2):
        kv = (2 * pair) // per_kv
        lanes = slice(pair * 2 * HEAD, (pair + 1) * 2 * HEAD)
        q = q_ref[:, lanes]
        spread = []
        for side in range(2):
            keys = k_ref[kv, side, pl.ds(begin, span), :]
            scores = lax.dot_general(
                q, keys, (((1,), (1,)), ((), ())), preferred_element_type=F32
            ) * (1.0 / math.sqrt(HEAD))
            scores = jnp.where(allowed, scores, -1e30)
            sink = sink_ref[2 * pair + side]
            row_top = jnp.maximum(jnp.max(scores, axis=-1, keepdims=True), sink)
            expo = jnp.exp(scores - row_top)
            denominator = jnp.sum(expo, axis=-1, keepdims=True) + jnp.exp(sink - row_top)
            spread.append((expo / denominator).astype(BF16))
        context = jnp.dot(
            spread[0], v_ref[kv, 0, pl.ds(begin, span), :], preferred_element_type=F32
        ) + jnp.dot(spread[1], v_ref[kv, 1, pl.ds(begin, span), :], preferred_element_type=F32)
        out_ref[:, lanes] = context.astype(BF16)


def attention(slab_index, sinks, queries, keys, values):
    rows, width = queries.shape
    heads = width // HEAD
    kv_count = keys.shape[0]
    return pl.pallas_call(
        functools.partial(attention_kernel, heads=heads, kv_count=kv_count),
        grid=(rows // WIN,),
        out_shape=jax.ShapeDtypeStruct((rows, width), BF16),
        in_specs=[
            pl.BlockSpec(memory_space=pltpu.SMEM),
            pl.BlockSpec(memory_space=pltpu.SMEM),
            pl.BlockSpec((WIN, width), lambda i: (i, 0)),
            full(keys.shape),
            full(values.shape),
        ],
        out_specs=pl.BlockSpec((WIN, width), lambda i: (i, 0)),
        compiler_params=params("arbitrary"),
        cost_estimate=cost(4e9, 2e6),
        name="attention",
    )(slab_index, sinks, queries, keys, values)


def both_sides(x, kv_count):
    rows = x.shape[0]
    heads = x.reshape(rows, kv_count, HEAD).transpose(1, 0, 2)
    zero = jnp.zeros_like(heads)
    return jnp.stack(
        [jnp.concatenate([heads, zero], 2), jnp.concatenate([zero, heads], 2)], axis=1
    )


def project_kernel(bit_ref, ctx_ref, w_ref, out_ref, *, width):
    out_ref[0] = jnp.dot(
        ctx_ref[...], w_ref[:, 0:width], preferred_element_type=F32
    ).astype(out_ref.dtype)


def project(bit, context, out_weight, start, width, block):
    rows, depth = context.shape
    half = rows // 2
    return pl.pallas_call(
        functools.partial(project_kernel, width=width),
        grid_spec=pltpu.PrefetchScalarGridSpec(
            num_scalar_prefetch=1,
            grid=(2,),
            in_specs=[
                pl.BlockSpec((half, depth), lambda i, bit_ref: (1 - i - bit_ref[0] + 2 * i * bit_ref[0], 0)),
                pl.BlockSpec((depth, block), lambda i, bit_ref: (0, start // block)),
            ],
            out_specs=pl.BlockSpec((1, half, width), lambda i, bit_ref: (i, 0, 0)),
        ),
        out_shape=jax.ShapeDtypeStruct((2, half, width), BF16),
        compiler_params=params("arbitrary"),
        cost_estimate=cost(2 * rows * depth * width, 2 * depth * width),
        name="project",
    )(bit, context, out_weight)


def enter_kernel(
    *refs, first, last, orders, slabs, experts, cap, rows, width
):
    refs = list(refs)
    near_ref, far_ref, place_ref, gain_ref, wg_ref, wu_ref = refs[:6]
    refs = refs[6:]
    if not first:
        acc_in, ss_in = refs[:2]
        refs = refs[2:]
    if last:
        hidden_ref, = refs[:1]
        refs = refs[1:]
        x_ref, ss_ref = refs
    else:
        acc_ref, ss_ref = refs[:2]
        x_ref, = refs[2:]
    e = pl.program_id(0)
    half = slabs // 2

    @pl.when(e == 0)
    def _():
        for n in range(slabs):
            source = near_ref if n < half else far_ref
            at = orders[n % half]
            x = jnp.dot(place_ref[n], source[at], preferred_element_type=F32)
            ss = jnp.sum(x * x, axis=1, keepdims=True)
            x = (x * gain_ref[...]).astype(BF16)
            for k in range(experts):
                part = slice(n * cap, (n + 1) * cap)
                x_ref[k, part, :] = x[k * cap : (k + 1) * cap]
                new = jnp.broadcast_to(ss[k * cap : (k + 1) * cap], (cap, LANES))
                if not first:
                    new = new + ss_in[k, part, :]
                ss_ref[k, part, :] = new

    x = x_ref[e]
    units = wg_ref.shape[2]
    gate_acc = jnp.dot(x, wg_ref[0], preferred_element_type=F32)
    up_acc = jnp.dot(x, wu_ref[0], preferred_element_type=F32)
    if not first:
        gate_acc = gate_acc + acc_in[0, :, 0:units]
        up_acc = up_acc + acc_in[0, :, units : 2 * units]
    if not last:
        acc_ref[0, :, 0:units] = gate_acc
        acc_ref[0, :, units : 2 * units] = up_acc
    else:
        total = last
        scale = lax.rsqrt(ss_ref[e][:, 0:1] * (1.0 / total) + 1e-05)
        gate_acc = jnp.minimum(gate_acc * scale, 7.0)
        up_acc = jnp.clip(up_acc * scale, -7.0, 7.0)
        hidden_ref[0] = (
            (up_acc + 1.0) * gate_acc / (1.0 + jnp.exp(-1.702 * gate_acc))
        ).astype(BF16)


def enter(near, far, place, gain, gate_proj, up_proj, carry, orders, start, last):
    half, rows, width = near.shape
    slabs, all_slots, _ = place.shape
    experts, total, units = gate_proj.shape
    cap = all_slots // experts
    slots = slabs * cap
    first = carry is None
    at = start // width
    weight_spec = pl.BlockSpec((1, width, units), lambda e: (e, at, 0))
    in_specs = [full(near.shape), full(far.shape), full(place.shape), full(gain.shape)]
    in_specs += [weight_spec, weight_spec]
    operands = [near, far, place, gain, gate_proj, up_proj]
    acc_spec = pl.BlockSpec((1, slots, 2 * units), lambda e: (e, 0, 0))
    ss_shape = (experts, slots, LANES)
    aliases = {}
    if not first:
        in_specs += [acc_spec, full(ss_shape)]
        operands += list(carry)
        if not last:
            aliases = {6: 0}
    scratch = [pltpu.VMEM((experts, slots, width), BF16)]
    if last:
        out_shape = jax.ShapeDtypeStruct((experts, slots, units), BF16)
        out_specs = pl.BlockSpec((1, slots, units), lambda e: (e, 0, 0))
        scratch += [pltpu.VMEM(ss_shape, F32)]
    else:
        out_shape = (
            jax.ShapeDtypeStruct((experts, slots, 2 * units), F32),
            jax.ShapeDtypeStruct(ss_shape, F32),
        )
        out_specs = (acc_spec, full(ss_shape))
    return pl.pallas_call(
        functools.partial(
            enter_kernel,
            first=first,
            last=total if last else 0,
            orders=orders,
            slabs=slabs,
            experts=experts,
            cap=cap,
            rows=rows,
            width=width,
        ),
        grid=(experts,),
        out_shape=out_shape,
        in_specs=in_specs,
        out_specs=out_specs,
        scratch_shapes=scratch,
        input_output_aliases=aliases,
        compiler_params=params("arbitrary"),
        cost_estimate=cost(4 * experts * slots * width * units * 1.5, 4 * experts * width * units),
        name="enter",
    )(*operands)


def leave_kernel(
    hidden_ref, w_ref, gate_ref, turned_ref, near_ref, far_ref, part_ref,
    *, orders, slabs, experts, cap, width
):
    e = pl.program_id(0)
    out = jnp.dot(hidden_ref[0], w_ref[0, :, 0:width], preferred_element_type=F32)
    out = (out * gate_ref[0][:, 0:1]).astype(BF16)
    for k in range(experts):

        @pl.when(e == k)
        def _():
            for n in range(slabs):
                part_ref[n, k * cap : (k + 1) * cap, :] = out[n * cap : (n + 1) * cap]

    @pl.when(e == experts - 1)
    def _():
        for n in range(slabs):
            target = near_ref if n < slabs // 2 else far_ref
            target[orders[n % (slabs // 2)]] = jnp.dot(
                turned_ref[n], part_ref[n], preferred_element_type=F32
            ).astype(BF16)


def leave(hidden, down_proj, row_gate, turned, orders, start, width, block):
    experts, slots, units = hidden.shape
    slabs, rows, all_slots = turned.shape
    cap = all_slots // experts
    half = slabs // 2
    piece = jax.ShapeDtypeStruct((half, rows, width), BF16)
    return pl.pallas_call(
        functools.partial(
            leave_kernel, orders=orders, slabs=slabs, experts=experts, cap=cap, width=width
        ),
        grid=(experts,),
        out_shape=(piece, piece),
        in_specs=[
            pl.BlockSpec((1, slots, units), lambda e: (e, 0, 0)),
            pl.BlockSpec((1, units, block), lambda e: (e, 0, start // block)),
            pl.BlockSpec((1, slots, LANES), lambda e: (e, 0, 0)),
            full(turned.shape),
        ],
        out_specs=(full(piece.shape), full(piece.shape)),
        scratch_shapes=[pltpu.VMEM((slabs, experts * cap, width), BF16)],
        compiler_params=params("arbitrary"),
        cost_estimate=cost(3 * experts * slots * width * units, 2 * experts * width * units),
        name="leave",
    )(hidden, down_proj, row_gate, turned)


def add(a, b):
    return (a.astype(F32) + b.astype(F32)).astype(BF16)


def gather_slabs(x, order):
    buf = x[None]
    for bit in order:
        buf = jnp.concatenate([buf, swap(buf, "seq", bit)], axis=0)
    return buf


def scatter_slabs(buf, order):
    for bit in reversed(order):
        half = buf.shape[0] // 2
        buf = add(buf[:half], swap(buf[half:], "seq", bit))
    return buf[0]


def positions(order, bits):
    found = []
    for p in range(1 << len(bits)):
        xor = sum(bit for k, bit in enumerate(bits) if p >> k & 1)
        found.append(sum(1 << k for k, bit in enumerate(order) if xor & bit))
    return tuple(found)


def sum_half(send, keep, n_exp):
    keep = add(keep, swap(send, "exp", 1))
    bit = 2
    while bit < n_exp:
        other = swap(keep, "exp", bit)
        bit *= 2
        if bit < n_exp:
            keep = add(keep, other)
        else:
            return keep.astype(F32) + other.astype(F32)
    return keep.astype(F32)


def chunks_of(total):
    block = -(-total // (4 * LANES)) * LANES
    return [(s, min(block, total - s)) for s in range(0, total, block)], block


def on_device(
    queries,
    key_rows,
    value_rows,
    sink_logits,
    residual,
    out_weight,
    norm_gain,
    expert_ids,
    route_gates,
    gate_proj,
    up_proj,
    down_proj,
):
    rows = queries.shape[0]
    half = rows // 2
    local_heads = queries.shape[1] // HEAD
    per_group = HQ // HK
    column = lax.axis_index("exp")
    slab_index = lax.axis_index("seq")
    n_exp = lax.axis_size("exp")
    slabs = lax.axis_size("seq")
    experts = gate_proj.shape[0]
    cap = 3 * rows * TOP // (2 * experts * slabs)
    total = residual.shape[1]
    low_bit = column % 2
    bit = low_bit[None].astype(jnp.int32)
    bits = [b for b in (1 << k for k in range(1, 31)) if b < slabs]

    kv_count = max(1, local_heads // per_group)
    kv_start = column * local_heads // per_group
    key_sel = lax.dynamic_slice_in_dim(key_rows, kv_start * HEAD, kv_count * HEAD, 1)
    value_sel = lax.dynamic_slice_in_dim(value_rows, kv_start * HEAD, kv_count * HEAD, 1)
    tail = jnp.concatenate([key_sel[rows - WIN :], value_sel[rows - WIN :]], axis=1)
    tail = lax.ppermute(tail, "seq", [(i, i + 1) for i in range(slabs - 1)])
    key_full = jnp.concatenate([tail[:, : kv_count * HEAD], key_sel], 0)
    value_full = jnp.concatenate([tail[:, kv_count * HEAD :], value_sel], 0)
    context = attention(
        slab_index[None].astype(jnp.int32),
        sink_logits,
        queries,
        both_sides(key_full, kv_count),
        both_sides(value_full, kv_count),
    )

    def halves(x):
        kept = lax.dynamic_slice_in_dim(x, low_bit * half, half, 0)
        other = lax.dynamic_slice_in_dim(x, (1 - low_bit) * half, half, 0)
        return kept, other

    meta = jnp.concatenate([expert_ids.astype(F32), route_gates], axis=1)
    meta = jnp.concatenate(halves(meta), axis=0).T
    meta = gather_slabs(meta, bits + [1])
    first_expert = (slab_index * experts)[None].astype(jnp.int32)
    place, turned, row_gate = route(first_expert, meta, experts, cap)

    chunks, block = chunks_of(total)
    res_kept = lax.dynamic_slice_in_dim(residual, low_bit * half, half, 0)
    gain = norm_gain[None, :]
    carry = None
    mixed_kept = []
    for c, (start, width) in enumerate(chunks):
        parts = project(bit, context, out_weight, start, width, block)
        attn = sum_half(parts[0], parts[1], n_exp)
        kept = (res_kept[:, start : start + width].astype(F32) + attn).astype(BF16)
        mixed_kept.append(kept)
        mixed = jnp.concatenate([kept, swap(kept, "exp", 1)], axis=0)
        order = bits if c % 2 == 0 else bits[::-1]
        near = gather_slabs(mixed, order)
        far = swap(near, "seq", 1)
        carry = enter(
            near, far, place, gain[:, start : start + width], gate_proj, up_proj, carry,
            positions(order, bits), start, c == len(chunks) - 1,
        )
    hidden = carry
    done = []
    for c, (start, width) in enumerate(chunks):
        order = bits if c % 2 == 0 else bits[::-1]
        near, far = leave(
            hidden, down_proj, row_gate, turned, positions(order, bits), start, width, block
        )
        buf = add(near, swap(far, "seq", 1))
        own = scatter_slabs(buf, order)
        moe = sum_half(own[half:], own[:half], n_exp)
        kept = (mixed_kept[c].astype(F32) + moe).astype(BF16)
        done.append((kept, swap(kept, "exp", 1)))
    mine = jnp.concatenate([d[0] for d in done], axis=1)
    theirs = jnp.concatenate([d[1] for d in done], axis=1)
    flipped = low_bit == 1
    return jnp.concatenate(
        [jnp.where(flipped, theirs, mine), jnp.where(flipped, mine, theirs)], axis=0
    )


def solution(mesh):
    return jax.shard_map(
        on_device,
        mesh=mesh,
        in_specs=(
            P("seq", "exp"),
            P("seq", None),
            P("seq", None),
            P("exp"),
            P("seq", None),
            P("exp", None),
            P(),
            P("seq", None),
            P("seq", None),
            P("seq", None, "exp"),
            P("seq", None, "exp"),
            P("seq", "exp", None),
        ),
        out_specs=P("seq", None),
        check_vma=False,
    )
```
